256 devices in a mesh: tp: 4 (over x), dp: 64 (over z, y, core).
Axes of the slice: x: 4, y: 4, z: 8, core: 2. Of those that a mesh axis runs over, the one named last changes fastest.
Arguments:
- g_qkv: bfloat16 [64, 512, 16, 3, 64], P('dp', None, 'tp')
- g_out: bfloat16 [64, 1024, 512], P('dp', 'tp')
- g_up: bfloat16 [64, 512, 2048], P('dp', None, 'tp')
- g_down: bfloat16 [64, 2048, 512], P('dp', 'tp')
- g_norms: bfloat16 [64, 6, 512], P('dp')
- master: float32 [4, 1051648], P('tp', 'dp')
- mom_one: float32 [4, 1051648], P('tp', 'dp')
- mom_two: float32 [4, 1051648], P('tp', 'dp')
Outputs:
- output 1: bfloat16 [512, 16, 3, 64], P(None, 'tp')
- output 2: bfloat16 [1024, 512], P('tp')
- output 3: bfloat16 [512, 2048], P(None, 'tp')
- output 4: bfloat16 [2048, 512], P('tp')
- output 5: bfloat16 [6, 512], replicated
- output 6: float32 [4, 1051648], P('tp', 'dp')
- output 7: float32 [4, 1051648], P('tp', 'dp')
- output 8: float32 [4, 1051648], P('tp', 'dp')
- output 9: float32 [], replicated
All inputs are finite; a program needn't handle non-finite values.
Results may differ from the reference program's by a relative error of at most 0.001.
Values are sent between devices in bfloat16 or wider.
A program may use at most 768 MiB of HBM per device.

```python
import jax
import jax.numpy as jnp
from jax import lax

WIDTH = 512
HEADS = 16
KV_HEADS = 16
HEAD = 64
FF_RED = 2048
TP_SIZE = 4
DP_SIZE = 64
STEP = 20

QKV_SLOTS = HEADS // KV_HEADS + 2
KV_LOCAL = KV_HEADS // TP_SIZE
FF_LOCAL = FF_RED // TP_SIZE
QKV_END = WIDTH * KV_LOCAL * QKV_SLOTS * HEAD
OUT_END = QKV_END + (HEADS * HEAD // TP_SIZE) * WIDTH
UP_END = OUT_END + WIDTH * FF_LOCAL
MAT_COUNT = UP_END + FF_LOCAL * WIDTH
LN_COUNT = 6 * WIDTH
FLAT_COUNT = MAT_COUNT + LN_COUNT
BETA_ONE = 0.9
BETA_TWO = 0.95
ADAM_EPS = 1e-8
DECAY = 0.1
LEARN_RATE = 1e-4
MAX_NORM = 1.0
NORM_EPS = 1e-6
BIAS_ONE = 1.0 - BETA_ONE ** STEP
BIAS_TWO = 1.0 - BETA_TWO ** STEP
GRAD_MAT_STD = (8.0 * DP_SIZE / (TP_SIZE * MAT_COUNT)) ** 0.5
GRAD_LN_STD = (8.0 * DP_SIZE / LN_COUNT) ** 0.5
CLIP_MAT_STD = (0.5 / (TP_SIZE * MAT_COUNT)) ** 0.5
CLIP_LN_STD = (0.5 / LN_COUNT) ** 0.5


def to_flat(w_qkv, w_out, w_up, w_down, w_norms):
    qkv_rows = w_qkv.reshape(WIDTH, TP_SIZE, KV_LOCAL, QKV_SLOTS, HEAD).transpose(1, 0, 2, 3, 4).reshape(TP_SIZE, QKV_END)
    out_rows = w_out.reshape(TP_SIZE, OUT_END - QKV_END)
    up_rows = w_up.reshape(WIDTH, TP_SIZE, FF_LOCAL).transpose(1, 0, 2).reshape(TP_SIZE, UP_END - OUT_END)
    down_rows = w_down.reshape(TP_SIZE, MAT_COUNT - UP_END)
    norm_rows = jnp.broadcast_to(w_norms.reshape(1, LN_COUNT), (TP_SIZE, LN_COUNT))
    return jnp.concatenate([qkv_rows, out_rows, up_rows, down_rows, norm_rows], axis=1)


def from_flat(flat):
    p_qkv = flat[:, :QKV_END].reshape(TP_SIZE, WIDTH, KV_LOCAL, QKV_SLOTS, HEAD).transpose(1, 0, 2, 3, 4).reshape(WIDTH, KV_HEADS, QKV_SLOTS, HEAD)
    p_out = flat[:, QKV_END:OUT_END].reshape(HEADS * HEAD, WIDTH)
    p_up = flat[:, OUT_END:UP_END].reshape(TP_SIZE, WIDTH, FF_LOCAL).transpose(1, 0, 2).reshape(WIDTH, FF_RED)
    p_down = flat[:, UP_END:MAT_COUNT].reshape(FF_RED, WIDTH)
    p_norms = flat[0, MAT_COUNT:].reshape(6, WIDTH)
    return p_qkv, p_out, p_up, p_down, p_norms


def replica_mean(grad):
    total = lax.fori_loop(0, DP_SIZE, lambda index, running: running + grad[index].astype(jnp.float32), jnp.zeros(grad.shape[1:], jnp.float32))
    return total / DP_SIZE


def draw_replicas(key, shape, scale):
    def one_replica(sub_key):
        return (jax.random.normal(sub_key, shape, jnp.float32) * scale).astype(jnp.bfloat16)
    return lax.map(one_replica, jax.random.split(key, DP_SIZE))


def setup_inputs(seed: int = 0) -> dict:
    keys = jax.random.split(jax.random.key(seed), 16)
    qkv_shape = (WIDTH, KV_HEADS, QKV_SLOTS, HEAD)
    out_shape = (HEADS * HEAD, WIDTH)
    up_shape = (WIDTH, FF_RED)
    down_shape = (FF_RED, WIDTH)
    g_qkv = draw_replicas(keys[0], qkv_shape, GRAD_MAT_STD)
    g_out = draw_replicas(keys[1], out_shape, GRAD_MAT_STD)
    g_up = draw_replicas(keys[2], up_shape, GRAD_MAT_STD)
    g_down = draw_replicas(keys[3], down_shape, GRAD_MAT_STD)
    g_norms = draw_replicas(keys[4], (6, WIDTH), GRAD_LN_STD)
    w_qkv = jax.random.normal(keys[5], qkv_shape, jnp.float32) * WIDTH ** -0.5
    w_out = jax.random.normal(keys[6], out_shape, jnp.float32) * (HEADS * HEAD) ** -0.5
    w_up = jax.random.normal(keys[7], up_shape, jnp.float32) * WIDTH ** -0.5
    w_down = jax.random.normal(keys[8], down_shape, jnp.float32) * FF_RED ** -0.5
    norm_base = jnp.tile(jnp.array([1.0, 0.0], jnp.float32), 3).reshape(6, 1)
    w_norms = norm_base + 0.1 * jax.random.normal(keys[9], (6, WIDTH), jnp.float32)
    master = to_flat(w_qkv, w_out, w_up, w_down, w_norms)
    mom_mat = 0.2 * CLIP_MAT_STD * jax.random.normal(keys[10], (TP_SIZE, MAT_COUNT), jnp.float32)
    mom_ln = 0.2 * CLIP_LN_STD * jax.random.normal(keys[11], (1, LN_COUNT), jnp.float32)
    mom_one = jnp.concatenate([mom_mat, jnp.broadcast_to(mom_ln, (TP_SIZE, LN_COUNT))], axis=1)
    var_mat = CLIP_MAT_STD * CLIP_MAT_STD * jax.random.uniform(keys[12], (TP_SIZE, MAT_COUNT), jnp.float32, 0.5, 1.5)
    var_ln = CLIP_LN_STD * CLIP_LN_STD * jax.random.uniform(keys[13], (1, LN_COUNT), jnp.float32, 0.5, 1.5)
    mom_two = jnp.concatenate([var_mat, jnp.broadcast_to(var_ln, (TP_SIZE, LN_COUNT))], axis=1)
    return {"g_qkv": g_qkv, "g_out": g_out, "g_up": g_up, "g_down": g_down, "g_norms": g_norms, "master": master, "mom_one": mom_one, "mom_two": mom_two}


def reference(g_qkv, g_out, g_up, g_down, g_norms, master, mom_one, mom_two):
    means = [replica_mean(grad) for grad in (g_qkv, g_out, g_up, g_down, g_norms)]
    grad_norm = jnp.sqrt(sum(jnp.sum(mean_grad * mean_grad) for mean_grad in means))
    clip = jnp.minimum(1.0, MAX_NORM / (grad_norm + NORM_EPS))
    grad_flat = to_flat(means[0], means[1], means[2], means[3], means[4]) * clip
    is_matrix = (jnp.arange(FLAT_COUNT) < MAT_COUNT)[None, :]
    mom_one_new = BETA_ONE * mom_one + (1.0 - BETA_ONE) * grad_flat
    mom_two_new = BETA_TWO * mom_two + (1.0 - BETA_TWO) * grad_flat * grad_flat
    step_dir = (mom_one_new / BIAS_ONE) / (jnp.sqrt(mom_two_new / BIAS_TWO) + ADAM_EPS)
    master_new = master - LEARN_RATE * (step_dir + jnp.where(is_matrix, DECAY * master, 0.0))
    p_qkv, p_out, p_up, p_down, p_norms = from_flat(master_new.astype(jnp.bfloat16))
    return (p_qkv, p_out, p_up, p_down, p_norms, master_new, mom_one_new, mom_two_new, grad_norm)
```

```python
import jax
import jax.numpy as jnp
from jax import lax
from jax.experimental import pallas as pl
from jax.experimental.pallas import tpu as pltpu
from jax.sharding import PartitionSpec as P

STEP = 20
BETA_ONE = 0.9
BETA_TWO = 0.95
ADAM_EPS = 1e-8
DECAY = 0.1
LEARN_RATE = 1e-4
MAX_NORM = 1.0
NORM_EPS = 1e-6
BIAS_ONE = 1.0 - BETA_ONE ** STEP
BIAS_TWO = 1.0 - BETA_TWO ** STEP
ARG_SPECS = (P("dp", None, "tp", None, None), P("dp", "tp", None), P("dp", None, "tp"), P("dp", "tp", None), P("dp", None, None), P("tp", "dp"), P("tp", "dp"), P("tp", "dp"))
OUT_SPECS = (P(None, "tp", None, None), P("tp", None), P(None, "tp"), P("tp", None), P(None, None), P("tp", "dp"), P("tp", "dp"), P("tp", "dp"), P())

MESH = pl.DeviceIdType.MESH
F32 = jnp.float32
BF16 = jnp.bfloat16
LANES = 128
NZ, NY, NC, NX = 8, 4, 2, 4
NK = NY * NC
FLAT = 1051648
MAT = 1048576
PART = FLAT // (NZ * NK)
ROWS = FLAT // LANES
ZROWS = ROWS // NZ
PROWS, QROWS = 96, 48
WIN = PROWS + QROWS
FLATBUF = 8232
FULL = PART // LANES
REST = PART - FULL * LANES
PARTROWS = 136
QKV_ROWS, OUT_ROWS, UP_ROWS, DOWN_ROWS = 3072, 1024, 2048, 2048
OUT_AT = QKV_ROWS
UP_AT = OUT_AT + OUT_ROWS
DOWN_AT = UP_AT + UP_ROWS
NORM_AT = DOWN_AT + DOWN_ROWS


def window_row(k):
    return (k * ZROWS) // NK


def window_lane(k):
    return (k * (ZROWS * LANES // NK)) % LANES


def exchange_kernel(
    g_qkv, g_out, g_up, g_down, g_norms, master, mom_one, mom_two,
    gath_p, gath_q, master_new, m_new, v_new, norm_out,
    in_qkv, in_out, in_up, in_down, in_norms, st_master, st_one, st_two,
    rows_master, rows_one, rows_two, flat,
    send_p, recv_p, send_q, recv_q, sum_p, sum_p_in, sum_q, sum_q_in, win,
    sq_k, sq_z, sq_x,
    in_sem, p_send, p_recv, q_send, q_recv, p2_send, p2_recv, q2_send, q2_recv,
    nk_send, nk_recv, nz_send, nz_recv, nx_send, nx_recv,
    ap1_send, ap1_recv, ap2_send, ap2_recv, ap3_send, ap3_recv,
    aq1_send, aq1_recv, aq2_send, aq2_recv, aq3_send, aq3_recv,
):
    tp = lax.axis_index("tp")
    dp = lax.axis_index("dp")
    z, k = dp // NK, dp % NK
    y, c = k // NC, k % NC

    def z_at(d):
        return lax.rem(z + d, NZ)

    def y_at(d):
        return lax.rem(y + d, NY)

    def k_at(d):
        return y_at(d // NC) * NC + lax.rem(c + d % NC, NC)

    def dev(zz, kk):
        return (tp, zz * NK + kk)

    def rdma(src, dst, send, recv, device):
        return pltpu.make_async_remote_copy(src_ref=src, dst_ref=dst, send_sem=send, recv_sem=recv, device_id=device, device_id_type=MESH)

    loads = [
        pltpu.make_async_copy(src, dst, in_sem.at[i])
        for i, (src, dst) in enumerate((
            (g_qkv, in_qkv), (g_down, in_down), (g_up, in_up), (g_out, in_out), (g_norms, in_norms),
            (master, st_master), (mom_one, st_one), (mom_two, st_two)))
    ]
    for load in loads:
        load.start()

    barrier = pltpu.get_barrier_semaphore()
    peers = [dev(z_at(d), k) for d in range(1, NZ)] + [dev(z, k_at(d)) for d in range(1, NK)]
    peers += [(lax.rem(tp + d, NX), dp) for d in range(1, NX)]
    for peer in peers:
        pl.semaphore_signal(barrier, inc=1, device_id=peer, device_id_type=MESH)

    flat[ROWS:FLATBUF, :] = jnp.zeros((FLATBUF - ROWS, LANES), F32)
    loads[0].wait()
    for col in range(6):
        for blk in range(4):
            tile = in_qkv[col * 128:(col + 1) * 128, blk * 128:(blk + 1) * 128].astype(F32)
            flat[pl.ds(blk * 768 + col, 128, stride=6), :] = tile.T

    def spread(ref, start, count):
        def body(i, _):
            tile = ref[pl.ds(pl.multiple_of(i * 16, 16), 16), :].astype(F32)
            for col in range(4):
                flat[pl.ds(start + i * 64 + col, 16, stride=4), :] = tile[:, col * 128:(col + 1) * 128]
            return 0
        lax.fori_loop(0, count // 64, body, 0)

    loads[1].wait()
    spread(in_down, DOWN_AT, DOWN_ROWS)
    loads[2].wait()
    spread(in_up, UP_AT, UP_ROWS)
    loads[3].wait()
    spread(in_out, OUT_AT, OUT_ROWS)
    loads[4].wait()
    tile = in_norms[...].astype(F32)
    for col in range(4):
        flat[pl.ds(NORM_AT + col, 6, stride=4), :] = tile[:, col * 128:(col + 1) * 128]

    def pack(dz, _):
        base = z_at(dz) * ZROWS
        for dk in range(NK):
            start = base + window_row(k_at(dk))
            send_p[dk, dz] = flat[pl.ds(start, PROWS), :].astype(BF16)
            send_q[dz, dk] = flat[pl.ds(start + PROWS, QROWS), :].astype(BF16)
        return 0
    lax.fori_loop(0, NZ, pack, 0)

    pl.semaphore_wait(barrier, len(peers))

    copies_p = [rdma(send_p.at[d], recv_p.at[d], p_send.at[d], p_recv.at[d], dev(z, k_at(d))) for d in range(1, NK)]
    copies_q = [rdma(send_q.at[d], recv_q.at[d], q_send.at[d], q_recv.at[d], dev(z_at(d), k)) for d in range(1, NZ)]
    for order in (3, 2, 4, 1, 5, 0, 6):
        copies_p[order].start()
        copies_q[order].start()

    for i, (state, rows) in enumerate(((st_master, rows_master), (st_one, rows_one), (st_two, rows_two))):
        loads[5 + i].wait()
        rows[FULL:PARTROWS, :] = jnp.zeros((PARTROWS - FULL, LANES), F32)

        def lift(j, _, state=state, rows=rows):
            for u in range(8):
                rows[pl.ds(j * 8 + u, 1), :] = state[:, pl.ds(pl.multiple_of((j * 8 + u) * LANES, LANES), LANES)]
            return 0
        lax.fori_loop(0, FULL // 8, lift, 0)
        rows[FULL:FULL + 1, 0:REST] = state[:, FULL * LANES:PART]

    order = (4, 3, 5, 2, 6, 1, 7)
    for copy in copies_p:
        copy.wait_recv()
    copies_p2 = {d: rdma(sum_p.at[d], sum_p_in.at[d], p2_send.at[d], p2_recv.at[d], dev(z_at(d), k)) for d in order}
    ready = None
    for d in order + (0,):
        total = send_p[0, d].astype(F32)
        for e in range(1, NK):
            total += recv_p[e, d].astype(F32)
        sum_p[d] = total
        if ready is not None:
            copies_p2[ready].start()
        ready = d

    for copy in copies_q:
        copy.wait_recv()
    copies_q2 = {d: rdma(sum_q.at[d], sum_q_in.at[d], q2_send.at[d], q2_recv.at[d], dev(z, k_at(d))) for d in order}
    ready = None
    for d in order + (0,):
        total = send_q[0, d].astype(F32)
        for e in range(1, NZ):
            total += recv_q[e, d].astype(F32)
        sum_q[d] = total
        if ready is not None:
            copies_q2[ready].start()
        ready = d

    for copy in copies_q2.values():
        copy.wait_recv()
    total = sum_q[0]
    for d in range(1, NK):
        total += sum_q_in[d]
    win[PROWS:WIN, :] = total * (1.0 / (NZ * NK))
    for copy in copies_p2.values():
        copy.wait_recv()
    total = sum_p[0]
    for d in range(1, NZ):
        total += sum_p_in[d]
    win[0:PROWS, :] = total * (1.0 / (NZ * NK))

    lane_at = window_lane(k)
    row = lax.broadcasted_iota(jnp.int32, (WIN, LANES), 0)
    lane = lax.broadcasted_iota(jnp.int32, (WIN, LANES), 1)
    entry = row * LANES + lane - lane_at
    counted = (entry >= 0) & (entry < PART) & ((entry + dp * PART < MAT) | (tp == 0))
    grad = win[...]
    squares = jnp.where(counted, grad * grad, 0.0)
    sq_k[k] = jnp.sum(squares.reshape(WIN // 8, 8, LANES), axis=0)
    copies_nk = [rdma(sq_k.at[k], sq_k.at[k], nk_send.at[d], nk_recv.at[d], dev(z, k_at(d))) for d in range(1, NK)]
    for copy in copies_nk:
        copy.start()
    win[...] = pltpu.roll(grad, lax.rem(LANES - lane_at, LANES), axis=1)
    part_lane = lane[0:PARTROWS]
    mean = jnp.where(part_lane < LANES - lane_at, win[0:PARTROWS, :], win[1:PARTROWS + 1, :])
    index = row[0:PARTROWS] * LANES + part_lane
    mean = jnp.where(index < PART, mean, 0.0)
    is_matrix = index + dp * PART < MAT
    old_master = rows_master[...]
    decayed = jnp.where(is_matrix, DECAY * old_master, 0.0)
    for copy in copies_nk:
        copy.wait_recv()
    total = sq_k[0]
    for i in range(1, NK):
        total += sq_k[i]
    sq_z[z] = total
    copies_nz = [rdma(sq_z.at[z], sq_z.at[z], nz_send.at[d], nz_recv.at[d], dev(z_at(d), k)) for d in range(1, NZ)]
    for copy in copies_nz:
        copy.start()
    for copy in copies_nz:
        copy.wait_recv()
    total = sq_z[0]
    for i in range(1, NZ):
        total += sq_z[i]
    sq_x[tp] = total
    copies_nx = [rdma(sq_x.at[tp], sq_x.at[tp], nx_send.at[d], nx_recv.at[d], (lax.rem(tp + d, NX), dp)) for d in range(1, NX)]
    for copy in copies_nx:
        copy.start()
    for copy in copies_nx:
        copy.wait_recv()
    total = sq_x[0]
    for i in range(1, NX):
        total += sq_x[i]
    norm = jnp.sqrt(jnp.sum(jnp.sum(total, axis=1, keepdims=True), axis=0, keepdims=True))
    norm_out[...] = jnp.broadcast_to(norm, (8, LANES))
    clip = jnp.minimum(1.0, MAX_NORM / (norm + NORM_EPS))

    grad = mean * clip
    m = BETA_ONE * rows_one[...] + (1.0 - BETA_ONE) * grad
    v = BETA_TWO * rows_two[...] + (1.0 - BETA_TWO) * grad * grad
    step_dir = (m / BIAS_ONE) / (jnp.sqrt(v / BIAS_TWO) + ADAM_EPS)
    new = old_master - LEARN_RATE * (step_dir + decayed)
    win[8:8 + PARTROWS, :] = pltpu.roll(new, lane_at, axis=1)
    shifted = jnp.where(lane[0:PARTROWS] >= lane_at, win[8:8 + PARTROWS, :], win[7:7 + PARTROWS, :]).astype(BF16)
    gath_p[c, y, z] = shifted[0:PROWS]
    gath_q[c, z, y, 0:PARTROWS - PROWS] = shifted[PROWS:PARTROWS]
    gath_q[c, z, y, PARTROWS - PROWS:QROWS] = jnp.zeros((WIN - PARTROWS, LANES), BF16)

    partner = dev(z, y * NC + 1 - c)

    def forward_p(d):
        src = gath_p.at[c, y, lax.rem(z + NZ - d, NZ)]
        copies = [rdma(src, src, ap2_send.at[d, e], ap2_recv.at[d, e], dev(z, y_at(e) * NC + c)) for e in (1, 3, 2)]
        for copy in copies:
            copy.start()
        return copies

    own_p, own_q = gath_p.at[c, y, z], gath_q.at[c, z, y]
    near = (1, 7, 2, 6, 3, 5, 4)
    ap1 = {d: rdma(own_p, own_p, ap1_send.at[d], ap1_recv.at[d], dev(z_at(d), k)) for d in near}
    aq1 = {d: rdma(own_q, own_q, aq1_send.at[d], aq1_recv.at[d], dev(z, y_at(d) * NC + c)) for d in (1, 3, 2)}
    for copy in aq1.values():
        copy.start()
    for copy in ap1.values():
        copy.start()
    ap2 = forward_p(0)
    master_new[...] = new
    m_new[...] = m
    v_new[...] = v
    for copy in aq1.values():
        copy.wait_recv()
    q_slab = gath_q.at[c, z]
    aq2 = {d: rdma(q_slab, q_slab, aq2_send.at[d], aq2_recv.at[d], dev(z_at(d), k)) for d in near}
    for copy in aq2.values():
        copy.start()
    aq3 = [rdma(q_slab, q_slab, aq3_send.at[0], aq3_recv.at[0], partner)]
    aq3[0].start()
    for d in near:
        ap1[d].wait_recv()
        ap2 += forward_p(d)
    p_slab = gath_p.at[c, y]
    ap3 = [rdma(p_slab, p_slab, ap3_send.at[0], ap3_recv.at[0], partner)]
    ap3[0].start()
    for d in near:
        aq2[d].wait_recv()
        slab = gath_q.at[c, lax.rem(z + NZ - d, NZ)]
        aq3.append(rdma(slab, slab, aq3_send.at[d], aq3_recv.at[d], partner))
        aq3[-1].start()
    for i, e in enumerate((1, 3, 2)):
        for d in range(NZ):
            ap2[d * 3 + i].wait_recv()
        slab = gath_p.at[c, lax.rem(y + NY - e, NY)]
        ap3.append(rdma(slab, slab, ap3_send.at[e], ap3_recv.at[e], partner))
        ap3[-1].start()
    for copy in aq3 + ap3:
        copy.wait_recv()
    sent = copies_p + copies_q + list(copies_p2.values()) + list(copies_q2.values()) + copies_nk + copies_nz + copies_nx
    sent += list(ap1.values()) + list(aq1.values()) + ap2 + list(aq2.values()) + aq3 + ap3
    for copy in sent:
        copy.wait_send()


def split_kernel(
    gath_p, gath_q, master_rows, m_rows, v_rows,
    p_qkv, p_out, p_up, p_down, p_norms, master_new, m_new, v_new, flat,
):
    for rows, out in ((master_rows, master_new), (m_rows, m_new), (v_rows, v_new)):
        def drop(j, _, rows=rows, out=out):
            for u in range(8):
                out[:, pl.ds(pl.multiple_of((j * 8 + u) * LANES, LANES), LANES)] = rows[pl.ds(j * 8 + u, 1), :]
            return 0
        lax.fori_loop(0, FULL // 8, drop, 0)
        out[:, FULL * LANES:PART] = rows[FULL:FULL + 1, 0:REST]

    lane = lax.broadcasted_iota(jnp.int32, (8, LANES), 1)
    flat[0:8, :] = jnp.zeros((8, LANES), F32)

    def place(zz, _):
        for k in range(NK):
            yy, cc = k // NC, k % NC
            start = zz * ZROWS + window_row(k)
            block = gath_p[cc, yy, zz].astype(F32)
            if window_lane(k):
                head = jnp.where(lane >= window_lane(k), block[0:8], flat[pl.ds(start, 8), :])
                row = lax.broadcasted_iota(jnp.int32, (8, LANES), 0)
                head = jnp.where(row == 0, head, block[0:8])
                flat[pl.ds(start, 8), :] = head
                flat[pl.ds(start + 8, PROWS - 8), :] = block[8:]
            else:
                flat[pl.ds(start, PROWS), :] = block
            flat[pl.ds(start + PROWS, QROWS), :] = gath_q[cc, zz, yy].astype(F32)
        return 0
    lax.fori_loop(0, NZ, place, 0)

    def collect(ref, start, count):
        def body(i, _):
            for col in range(4):
                tile = flat[pl.ds(start + i * 64 + col, 16, stride=4), :]
                ref[pl.ds(pl.multiple_of(i * 16, 16), 16), col * 128:(col + 1) * 128] = tile.astype(BF16)
            return 0
        lax.fori_loop(0, count // 64, body, 0)

    collect(p_out, OUT_AT, OUT_ROWS)
    collect(p_up, UP_AT, UP_ROWS)
    collect(p_down, DOWN_AT, DOWN_ROWS)
    for col in range(4):
        p_norms[:, col * 128:(col + 1) * 128] = flat[pl.ds(NORM_AT + col, 6, stride=4), :].astype(BF16)
    for col in range(6):
        for blk in range(4):
            tile = flat[pl.ds(blk * 768 + col, 128, stride=6), :]
            p_qkv[col * 128:(col + 1) * 128, blk * 128:(blk + 1) * 128] = tile.T.astype(BF16)


def solution(mesh):
    vmem = pl.BlockSpec(memory_space=pltpu.VMEM)
    anyspace = pl.BlockSpec(memory_space=pl.ANY)
    dma = pltpu.SemaphoreType.DMA

    def local_step(g_qkv, g_out, g_up, g_down, g_norms, master, mom_one, mom_two):
        qkv_t = g_qkv[0].transpose(1, 2, 3, 0).reshape(768, 512)
        state = jax.ShapeDtypeStruct((PARTROWS, LANES), F32)
        gath_p, gath_q, master_rows, m_rows, v_rows, norm = pl.pallas_call(
            exchange_kernel,
            out_shape=(
                jax.ShapeDtypeStruct((NC, NY, NZ, PROWS, LANES), BF16),
                jax.ShapeDtypeStruct((NC, NZ, NY, QROWS, LANES), BF16),
                state, state, state,
                jax.ShapeDtypeStruct((8, LANES), F32),
            ),
            in_specs=[anyspace] * 8,
            out_specs=(vmem,) * 6,
            scratch_shapes=[
                pltpu.VMEM((768, 512), BF16), pltpu.VMEM((256, 512), BF16), pltpu.VMEM((512, 512), BF16), pltpu.VMEM((512, 512), BF16), pltpu.VMEM((6, 512), BF16),
                pltpu.VMEM((1, PART), F32), pltpu.VMEM((1, PART), F32), pltpu.VMEM((1, PART), F32),
                pltpu.VMEM((PARTROWS, LANES), F32), pltpu.VMEM((PARTROWS, LANES), F32), pltpu.VMEM((PARTROWS, LANES), F32),
                pltpu.VMEM((FLATBUF, LANES), F32),
                pltpu.VMEM((NK, NZ, PROWS, LANES), BF16), pltpu.VMEM((NK, NZ, PROWS, LANES), BF16),
                pltpu.VMEM((NZ, NK, QROWS, LANES), BF16), pltpu.VMEM((NZ, NK, QROWS, LANES), BF16),
                pltpu.VMEM((NZ, PROWS, LANES), F32), pltpu.VMEM((NZ, PROWS, LANES), F32),
                pltpu.VMEM((NK, QROWS, LANES), F32), pltpu.VMEM((NK, QROWS, LANES), F32),
                pltpu.VMEM((WIN, LANES), F32),
                pltpu.VMEM((NK, 8, LANES), F32), pltpu.VMEM((NZ, 8, LANES), F32), pltpu.VMEM((NX, 8, LANES), F32),
                dma((8,)),
                dma((NK,)), dma((NK,)), dma((NZ,)), dma((NZ,)), dma((NZ,)), dma((NZ,)), dma((NK,)), dma((NK,)),
                dma((NK,)), dma((NK,)), dma((NZ,)), dma((NZ,)), dma((NX,)), dma((NX,)),
                dma((NZ,)), dma((NZ,)), dma((NZ, NY)), dma((NZ, NY)), dma((NY,)), dma((NY,)),
                dma((NY,)), dma((NY,)), dma((NZ,)), dma((NZ,)), dma((NZ,)), dma((NZ,)),
            ],
            compiler_params=pltpu.CompilerParams(collective_id=0, has_side_effects=True),
            name="exchange",
        )(qkv_t, g_out[0], g_up[0], g_down[0], g_norms[0], master, mom_one, mom_two)
        row = jax.ShapeDtypeStruct((1, PART), F32)
        p_qkv, p_out, p_up, p_down, p_norms, master_new, m_new, v_new = pl.pallas_call(
            split_kernel,
            out_shape=(
                jax.ShapeDtypeStruct((768, 512), BF16), jax.ShapeDtypeStruct((256, 512), BF16),
                jax.ShapeDtypeStruct((512, 512), BF16), jax.ShapeDtypeStruct((512, 512), BF16),
                jax.ShapeDtypeStruct((6, 512), BF16), row, row, row,
            ),
            in_specs=[vmem] * 5,
            out_specs=(vmem,) * 8,
            scratch_shapes=[pltpu.VMEM((FLATBUF, LANES), F32)],
            name="split",
        )(gath_p, gath_q, master_rows, m_rows, v_rows)
        p_qkv = p_qkv.reshape(4, 3, 64, 512).transpose(3, 0, 1, 2)
        return p_qkv, p_out, p_up, p_down, p_norms, master_new, m_new, v_new, norm[0, 0]

    return jax.shard_map(local_step, mesh=mesh, in_specs=ARG_SPECS, out_specs=OUT_SPECS, check_vma=False)
```

```python
import jax
import jax.numpy as jnp
from jax import lax
from jax.experimental import pallas as pl
from jax.experimental.pallas import tpu as pltpu
from jax.sharding import PartitionSpec as P

STEP = 20
BETA_ONE = 0.9
BETA_TWO = 0.95
ADAM_EPS = 1e-8
DECAY = 0.1
LEARN_RATE = 1e-4
MAX_NORM = 1.0
NORM_EPS = 1e-6
BIAS_ONE = 1.0 - BETA_ONE ** STEP
BIAS_TWO = 1.0 - BETA_TWO ** STEP
ARG_SPECS = (P("dp", None, "tp", None, None), P("dp", "tp", None), P("dp", None, "tp"), P("dp", "tp", None), P("dp", None, None), P("tp", "dp"), P("tp", "dp"), P("tp", "dp"))
OUT_SPECS = (P(None, "tp", None, None), P("tp", None), P(None, "tp"), P("tp", None), P(None, None), P("tp", "dp"), P("tp", "dp"), P("tp", "dp"), P())

MESH = pl.DeviceIdType.MESH
F32 = jnp.float32
BF16 = jnp.bfloat16
LANES = 128
NZ, NY, NC, NX = 8, 4, 2, 4
NK = NY * NC
NNEAR = NX * NK
FLAT = 1051648
MAT = 1048576
PART = FLAT // (NZ * NK)
ROWS = FLAT // LANES
ZROWS = ROWS // NZ
FULL = PART // LANES
REST = PART - FULL * LANES
WIN = 136
FLATBUF = 8224
PCHUNKS = (40, 40, 16)
QROWS = WIN - sum(PCHUNKS)
GP = 104
GQ = WIN - GP
QKV_ROWS, OUT_ROWS, UP_ROWS, DOWN_ROWS = 3072, 1024, 2048, 2048
OUT_AT = QKV_ROWS
UP_AT = OUT_AT + OUT_ROWS
DOWN_AT = UP_AT + UP_ROWS
NORM_AT = DOWN_AT + DOWN_ROWS
FAR = (4, 3, 5, 2, 6, 1, 7)
NEAR = (1, 7, 2, 6, 3, 5, 4)
KFAR = (4, 5, 2, 6, 3, 7, 1)


def window_row(k):
    return (k * ZROWS) // NK


def window_lane(k):
    return (k * (ZROWS * LANES // NK)) % LANES


def sum_all(terms):
    total = terms[0]
    for term in terms[1:]:
        total = total + term
    return total


def exchange_kernel(names, *refs):
    r = dict(zip(names, refs))
    tp = lax.axis_index("tp")
    dp = lax.axis_index("dp")
    z, k = dp // NK, dp % NK
    y, c = k // NC, k % NC
    flat = r["flat"]

    def z_at(d):
        return lax.rem(z + d, NZ)

    def y_at(d):
        return lax.rem(y + d, NY)

    def k_at(d):
        return y_at(d // NC) * NC + lax.rem(c + d % NC, NC)

    def dev(zz, kk):
        return (tp, zz * NK + kk)

    def near_dev(d):
        return (lax.rem(tp + d // NK, NX), z * NK + k_at(d % NK))

    def rdma(src, dst, sems, index, device):
        return pltpu.make_async_remote_copy(
            src_ref=src, dst_ref=dst, send_sem=r[sems + "_send"].at[index], recv_sem=r[sems + "_recv"].at[index],
            device_id=device, device_id_type=MESH)
    loads = {
        name: pltpu.make_async_copy(r[name], r["in_" + name], r["in_sem"].at[i])
        for i, name in enumerate(("qkv", "down", "up", "out", "norms", "master", "one", "two"))
    }
    for load in loads.values():
        load.start()

    barrier = pltpu.get_barrier_semaphore()
    peers = [dev(z_at(d), k) for d in range(1, NZ)] + [near_dev(d) for d in range(1, NNEAR)]
    for peer in peers:
        pl.semaphore_signal(barrier, inc=1, device_id=peer, device_id_type=MESH)
    flat[ROWS:FLATBUF, :] = jnp.zeros((FLATBUF - ROWS, LANES), F32)
    loads["qkv"].wait()
    for col in range(6):
        for blk in range(4):
            tile = r["in_qkv"][col * 128:(col + 1) * 128, blk * 128:(blk + 1) * 128].astype(F32)
            flat[pl.ds(blk * 768 + col, 128, stride=6), :] = tile.T

    def spread(name, start, count):
        loads[name].wait()
        ref = r["in_" + name]

        def body(i, _):
            tile = ref[pl.ds(pl.multiple_of(i * 16, 16), 16), :].astype(F32)
            for col in range(4):
                flat[pl.ds(start + i * 64 + col, 16, stride=4), :] = tile[:, col * 128:(col + 1) * 128]
            return 0
        lax.fori_loop(0, count // 64, body, 0)
    spread("down", DOWN_AT, DOWN_ROWS)
    spread("up", UP_AT, UP_ROWS)
    spread("out", OUT_AT, OUT_ROWS)
    loads["norms"].wait()
    tile = r["in_norms"][...].astype(F32)
    for col in range(4):
        flat[pl.ds(NORM_AT + col, 6, stride=4), :] = tile[:, col * 128:(col + 1) * 128]

    send_q, recv_q, sum_q, in_q = r["send_q"], r["recv_q"], r["sum_q"], r["in_q"]
    qstart = sum(PCHUNKS)

    def pack_q(dz, _):
        for dk in range(NK):
            start = z_at(dz) * ZROWS + window_row(k_at(dk)) + qstart
            send_q[dz, dk] = flat[pl.ds(start, QROWS), :].astype(BF16)
        return 0
    lax.fori_loop(0, NZ, pack_q, 0)
    pl.semaphore_wait(barrier, len(peers))
    q_one = {d: rdma(send_q.at[d], recv_q.at[d], "q1", d, dev(z_at(d), k)) for d in FAR}
    for copy in q_one.values():
        copy.start()
    p_one = []
    row_at = 0
    for i, rows in enumerate(PCHUNKS):
        send_p = r[f"send_p{i}"]

        def pack_p(dz, _, rows=rows, row_at=row_at, send_p=send_p):
            for dk in range(NK):
                start = z_at(dz) * ZROWS + window_row(k_at(dk)) + row_at
                send_p[dk, dz] = flat[pl.ds(start, rows), :].astype(BF16)
            return 0
        lax.fori_loop(0, NZ, pack_p, 0)
        p_one.append({d: rdma(send_p.at[d], r[f"recv_p{i}"].at[d], f"p1{i}", d, dev(z, k_at(d))) for d in KFAR})
        for copy in p_one[i].values():
            copy.start()
        row_at += rows

    for name in ("master", "one", "two"):
        loads[name].wait()
        state, rows = r["in_" + name], r["rows_" + name]
        rows[FULL:WIN, :] = jnp.zeros((WIN - FULL, LANES), F32)

        def lift(j, _, state=state, rows=rows):
            for u in range(8):
                rows[pl.ds(j * 8 + u, 1), :] = state[:, pl.ds(pl.multiple_of((j * 8 + u) * LANES, LANES), LANES)]
            return 0
        lax.fori_loop(0, FULL // 8, lift, 0)
        rows[FULL:FULL + 1, 0:REST] = state[:, FULL * LANES:PART]

    def second(copies, send, recv, total, landed, sems, order, device):
        for copy in copies.values():
            copy.wait_recv()
        out = {d: rdma(total.at[d], landed.at[d], sems, d, device(d)) for d in order}
        ready = None
        for d in order + (0,):
            total[d] = sum_all([send[0, d].astype(F32)] + [recv[e, d].astype(F32) for e in range(1, 8)])
            if ready is not None:
                out[ready].start()
            ready = d
        return out

    p_two = []

    def second_p(i):
        p_two.append(second(p_one[i], r[f"send_p{i}"], r[f"recv_p{i}"], r[f"sum_p{i}"], r[f"in_p{i}"], f"p2{i}", FAR, lambda d: dev(z_at(d), k)))

    for i in range(len(PCHUNKS) - 1):
        second_p(i)
    q_two = second(q_one, send_q, recv_q, sum_q, in_q, "q2", KFAR, lambda d: dev(z, k_at(d)))
    second_p(len(PCHUNKS) - 1)

    lane_at = window_lane(k)
    win = r["win"]

    def finish(copies, total, landed, start, rows):
        for copy in copies.values():
            copy.wait_recv()
        mean = sum_all([total[0]] + [landed[d] for d in range(1, 8)]) * (1.0 / (NZ * NK))
        win[start:start + rows, :] = mean
        row = lax.broadcasted_iota(jnp.int32, (rows, LANES), 0) + start
        entry = row * LANES + lax.broadcasted_iota(jnp.int32, (rows, LANES), 1) - lane_at
        counted = (entry >= 0) & (entry < PART) & ((entry + dp * PART < MAT) | (tp == 0))
        squares = jnp.where(counted, mean * mean, 0.0)
        return jnp.sum(squares.reshape(rows // 8, 8, LANES), axis=0)

    squares = []
    row_at = 0
    for i, rows in enumerate(PCHUNKS):
        if i == len(PCHUNKS) - 1:
            squares.append(finish(q_two, sum_q, in_q, qstart, QROWS))
        squares.append(finish(p_two[i], r[f"sum_p{i}"], r[f"in_p{i}"], row_at, rows))
        row_at += rows

    sq_near, sq_z = r["sq_near"], r["sq_z"]
    me = tp * NK + k
    sq_near[me] = jnp.sum(sum_all(squares), axis=0, keepdims=True)
    near = {d: rdma(sq_near.at[me], sq_near.at[me], "near", d, near_dev(d)) for d in range(1, NNEAR)}
    for copy in near.values():
        copy.start()
    lane = lax.broadcasted_iota(jnp.int32, (WIN, LANES), 1)
    row = lax.broadcasted_iota(jnp.int32, (WIN, LANES), 0)
    win[0:WIN, :] = pltpu.roll(win[0:WIN, :], lax.rem(LANES - lane_at, LANES), axis=1)
    mean = jnp.where(lane < LANES - lane_at, win[0:WIN, :], win[1:WIN + 1, :])
    index = row * LANES + lane
    mean = jnp.where(index < PART, mean, 0.0)
    is_matrix = index + dp * PART < MAT
    old_master = r["rows_master"][...]
    decayed = jnp.where(is_matrix, DECAY * old_master, 0.0)
    for copy in near.values():
        copy.wait_recv()
    sq_z[z] = sum_all([sq_near[i] for i in range(NNEAR)])
    across = {d: rdma(sq_z.at[z], sq_z.at[z], "across", d, dev(z_at(d), k)) for d in FAR}
    for copy in across.values():
        copy.start()
    for copy in across.values():
        copy.wait_recv()
    norm = jnp.sqrt(jnp.sum(sum_all([sq_z[i] for i in range(NZ)]), axis=1, keepdims=True))
    r["norm"][...] = norm
    clip = jnp.minimum(1.0, MAX_NORM / (norm + NORM_EPS))

    grad = mean * clip
    m = BETA_ONE * r["rows_one"][...] + (1.0 - BETA_ONE) * grad
    v = BETA_TWO * r["rows_two"][...] + (1.0 - BETA_TWO) * grad * grad
    step_dir = (m / BIAS_ONE) / (jnp.sqrt(v / BIAS_TWO) + ADAM_EPS)
    new = old_master - LEARN_RATE * (step_dir + decayed)
    win[8:8 + WIN, :] = pltpu.roll(new, lane_at, axis=1)
    shifted = jnp.where(lane >= lane_at, win[8:8 + WIN, :], win[7:7 + WIN, :]).astype(BF16)
    gath_p, gath_q = r["gath_p"], r["gath_q"]
    gath_p[z, c, y] = shifted[0:GP]
    gath_q[z, c, y] = shifted[GP:WIN]

    partner = dev(z, y * NC + 1 - c)
    to_y = (1, 3, 2)

    def from_z(d):
        return lax.rem(z + NZ - d, NZ)

    def from_y(d):
        return lax.rem(y + NY - d, NY)

    own_p, own_q = gath_p.at[z, c, y], gath_q.at[z, c, y]
    gq1 = {d: rdma(own_q, own_q, "gq1", d, dev(z, y_at(d) * NC + c)) for d in to_y}
    gp1 = {d: rdma(own_p, own_p, "gp1", d, dev(z_at(d), k)) for d in NEAR}
    gp2, gp3, gq3 = {}, {}, {}

    def relay(zd, yd):
        src = gath_p.at[from_z(zd), c, from_y(yd)]
        gp3[zd, yd] = rdma(src, src, "gp3", (zd, yd), partner)
        gp3[zd, yd].start()

    def spread_p(zd):
        src = gath_p.at[from_z(zd), c, y]
        for yd in to_y:
            gp2[zd, yd] = rdma(src, src, "gp2", (zd, yd), dev(z, y_at(yd) * NC + c))
            gp2[zd, yd].start()
        relay(zd, 0)

    for copy in gq1.values():
        copy.start()
    for copy in gp1.values():
        copy.start()
    spread_p(0)
    r["master_new"][...] = new
    r["m_new"][...] = m
    r["v_new"][...] = v
    for zd in NEAR[:2]:
        gp1[zd].wait_recv()
        spread_p(zd)
    for copy in gq1.values():
        copy.wait_recv()
    slab = gath_q.at[z, c]
    gq2 = {d: rdma(slab, slab, "gq2", d, dev(z_at(d), k)) for d in NEAR}
    for copy in gq2.values():
        copy.start()
    gq3[0] = rdma(slab, slab, "gq3", 0, partner)
    gq3[0].start()
    for zd in NEAR[2:]:
        gp1[zd].wait_recv()
        spread_p(zd)
    for zd in (0,) + NEAR[:-1]:
        for yd in to_y:
            gp2[zd, yd].wait_recv()
            relay(zd, yd)
    for zd in NEAR:
        gq2[zd].wait_recv()
        slab = gath_q.at[from_z(zd), c]
        gq3[zd] = rdma(slab, slab, "gq3", zd, partner)
        gq3[zd].start()
    for yd in to_y:
        gp2[NEAR[-1], yd].wait_recv()
        relay(NEAR[-1], yd)
    for copies in (gp3, gq3):
        for copy in copies.values():
            copy.wait_recv()
    for copies in [q_one, q_two, near, across, gq1, gp1, gp2, gp3, gq2, gq3] + p_one + p_two:
        for copy in copies.values():
            copy.wait_send()


def split_kernel(
    gath_p, gath_q, master_rows, m_rows, v_rows, norm_in,
    p_qkv, p_out, p_up, p_down, p_norms, master_new, m_new, v_new, norm_out,
    flat, out_qkv, out_out, out_up, out_down, out_norms, out_master, out_m, out_v, sem,
):
    norm_out[...] = norm_in[...]
    copies = []

    def flush(src, dst):
        copies.append(pltpu.make_async_copy(src, dst, sem.at[len(copies)]))
        copies[-1].start()

    for rows, out, dst in ((master_rows, out_master, master_new), (m_rows, out_m, m_new), (v_rows, out_v, v_new)):
        def drop(j, _, rows=rows, out=out):
            for u in range(8):
                out[:, pl.ds(pl.multiple_of((j * 8 + u) * LANES, LANES), LANES)] = rows[pl.ds(j * 8 + u, 1), :]
            return 0
        lax.fori_loop(0, FULL // 8, drop, 0)
        out[:, FULL * LANES:PART] = rows[FULL:FULL + 1, 0:REST]
        flush(out, dst)

    lane = lax.broadcasted_iota(jnp.int32, (8, LANES), 1)
    row = lax.broadcasted_iota(jnp.int32, (8, LANES), 0)

    def place(zz, _):
        for k in range(NK):
            yy, cc = k // NC, k % NC
            start = zz * ZROWS + window_row(k)
            block = gath_p[zz, cc, yy].astype(F32)
            head = block[0:8]
            if window_lane(k):
                head = jnp.where((row == 0) & (lane < window_lane(k)), flat[pl.ds(start, 8), :], head)
            flat[pl.ds(start, 8), :] = head
            flat[pl.ds(start + 8, GP - 8), :] = block[8:]
            flat[pl.ds(start + GP, GQ), :] = gath_q[zz, cc, yy].astype(F32)
        return 0

    def collect(ref, start, count):
        def body(i, _):
            for col in range(4):
                tile = flat[pl.ds(start + i * 64 + col, 16, stride=4), :]
                ref[pl.ds(pl.multiple_of(i * 16, 16), 16), col * 128:(col + 1) * 128] = tile.astype(BF16)
            return 0
        lax.fori_loop(0, count // 64, body, 0)

    lax.fori_loop(0, 3, place, 0)
    for col in range(6):
        for blk in range(4):
            tile = flat[pl.ds(blk * 768 + col, 128, stride=6), :]
            out_qkv[col * 128:(col + 1) * 128, blk * 128:(blk + 1) * 128] = tile.T.astype(BF16)
    flush(out_qkv, p_qkv)
    lax.fori_loop(3, 6, place, 0)
    collect(out_out, OUT_AT, OUT_ROWS)
    flush(out_out, p_out)
    collect(out_up, UP_AT, UP_ROWS)
    flush(out_up, p_up)
    lax.fori_loop(6, 8, place, 0)
    collect(out_down, DOWN_AT, DOWN_ROWS)
    for col in range(4):
        out_norms[:, col * 128:(col + 1) * 128] = flat[pl.ds(NORM_AT + col, 6, stride=4), :].astype(BF16)
    flush(out_norms, p_norms)
    flush(out_down, p_down)
    for copy in copies:
        copy.wait()


def solution(mesh):
    vmem = pl.BlockSpec(memory_space=pltpu.VMEM)
    hbm = pl.BlockSpec(memory_space=pltpu.HBM)
    dma = pltpu.SemaphoreType.DMA
    v = pltpu.VMEM

    scratch = {
        "in_qkv": v((768, 512), BF16), "in_out": v((256, 512), BF16), "in_up": v((512, 512), BF16),
        "in_down": v((512, 512), BF16), "in_norms": v((6, 512), BF16),
        "in_master": v((1, PART), F32), "in_one": v((1, PART), F32), "in_two": v((1, PART), F32),
        "rows_master": v((WIN, LANES), F32), "rows_one": v((WIN, LANES), F32), "rows_two": v((WIN, LANES), F32),
        "flat": v((FLATBUF, LANES), F32), "win": v((WIN + 8, LANES), F32),
        "send_q": v((NZ, NK, QROWS, LANES), BF16), "recv_q": v((NZ, NK, QROWS, LANES), BF16),
        "sum_q": v((NK, QROWS, LANES), F32), "in_q": v((NK, QROWS, LANES), F32),
        "sq_near": v((NNEAR, 1, LANES), F32), "sq_z": v((NZ, 1, LANES), F32),
        "in_sem": dma((8,)),
    }
    sems = {"q1": (NZ,), "q2": (NK,), "near": (NNEAR,), "across": (NZ,), "gq1": (NY,), "gq2": (NZ,), "gq3": (NZ,), "gp1": (NZ,), "gp2": (NZ, NY), "gp3": (NZ, NY)}
    for i, rows in enumerate(PCHUNKS):
        scratch[f"send_p{i}"] = v((NK, NZ, rows, LANES), BF16)
        scratch[f"recv_p{i}"] = v((NK, NZ, rows, LANES), BF16)
        scratch[f"sum_p{i}"] = v((NZ, rows, LANES), F32)
        scratch[f"in_p{i}"] = v((NZ, rows, LANES), F32)
        sems[f"p1{i}"] = (NK,)
        sems[f"p2{i}"] = (NZ,)
    for name, shape in sems.items():
        scratch[name + "_send"] = dma(shape)
        scratch[name + "_recv"] = dma(shape)
    operands = ("qkv", "out", "up", "down", "norms", "master", "one", "two")
    results = ("gath_p", "gath_q", "master_new", "m_new", "v_new", "norm")
    names = operands + results + tuple(scratch)

    def local_step(g_qkv, g_out, g_up, g_down, g_norms, master, mom_one, mom_two):
        qkv_t = g_qkv[0].transpose(1, 2, 3, 0).reshape(768, 512)
        state = jax.ShapeDtypeStruct((WIN, LANES), F32)
        one = jax.ShapeDtypeStruct((1, 1), F32)
        gathered = pl.pallas_call(
            lambda *refs: exchange_kernel(names, *refs),
            out_shape=(
                jax.ShapeDtypeStruct((NZ, NC, NY, GP, LANES), BF16),
                jax.ShapeDtypeStruct((NZ, NC, NY, GQ, LANES), BF16),
                state, state, state, one,
            ),
            in_specs=[hbm] * 8,
            out_specs=(vmem,) * 6,
            scratch_shapes=list(scratch.values()),
            compiler_params=pltpu.CompilerParams(collective_id=0, has_side_effects=True, vmem_limit_bytes=28 * 2**20),
            name="exchange",
        )(*[pltpu.with_memory_space_constraint(x, pltpu.HBM) for x in (qkv_t, g_out[0], g_up[0], g_down[0], g_norms[0], master, mom_one, mom_two)])
        shapes = [((768, 512), BF16), ((256, 512), BF16), ((512, 512), BF16), ((512, 512), BF16), ((6, 512), BF16)] + [((1, PART), F32)] * 3
        outs = pl.pallas_call(
            split_kernel,
            out_shape=tuple(jax.ShapeDtypeStruct(s, t) for s, t in shapes) + (one,),
            in_specs=[vmem] * 6,
            out_specs=(hbm,) * 8 + (vmem,),
            scratch_shapes=[v((FLATBUF, LANES), F32)] + [v(s, t) for s, t in shapes] + [dma((8,))],
            compiler_params=pltpu.CompilerParams(vmem_limit_bytes=20 * 2**20),
            name="split",
        )(*gathered)
        p_qkv = outs[0].reshape(4, 3, 64, 512).transpose(3, 0, 1, 2)
        return (p_qkv,) + outs[1:8] + (outs[8].reshape(()),)

    return jax.shard_map(local_step, mesh=mesh, in_specs=ARG_SPECS, out_specs=OUT_SPECS, check_vma=False)
```
